32 devices in a mesh: grp: 4 (over z), dev: 8 (over y, x, core).
Axes of the slice: x: 2, y: 2, z: 4, core: 2. Of those that a mesh axis runs over, the one named last changes fastest.
Arguments:
- atm_state: float32 [4, 8, 128, 1024], P('grp', 'dev'), may hold values from -6 to 6
- atm_nbrs: int32 [4, 8, 4, 1024], P('grp', 'dev'), may hold values from 0 to 1279
- atm_send: int32 [4, 8, 256], P('grp', 'dev'), may hold values from 0 to 1023
- atm_mix: float32 [4, 8, 1024], P('grp', 'dev'), may hold values from 0.2 to 0.6
- flux_weight: float32 [24, 128], replicated, may hold values from -0.5 to 0.5
- margin_counts: int32 [4, 8, 1024], P('grp', 'dev'), may hold values from 1 to 4, 1536 in all within a row
- margin_weight: float32 [4, 8, 1536], P('grp', 'dev'), may hold values from 0.05 to 1
- block_owner: int32 [4, 8, 12, 1], P('grp', 'dev'), may hold values from 0 to 1, as said below
- recv_cols: int32 [4, 8, 2, 12, 128], P('grp', 'dev'), may hold values from 0 to 2047
- ocn_state: float32 [4, 8, 80, 2048], P('grp', 'dev'), may hold values from -6 to 6
- ocn_nbrs: int32 [4, 8, 6, 2048], P('grp', 'dev'), may hold values from 0 to 2303
- ocn_send: int32 [4, 8, 256], P('grp', 'dev'), may hold values from 0 to 2047
- ocn_mix: float32 [4, 8, 2048], P('grp', 'dev'), may hold values from 0.1 to 0.4
- force_weight: float32 [80, 24], replicated, may hold values from -1.25 to 1.25
- ret_weight: float32 [12, 80], replicated, may hold values from -0.625 to 0.625
Outputs:
- atm_next: float32 [4, 8, 128, 1024], P('grp', 'dev')
- ocn_next: float32 [4, 8, 80, 2048], P('grp', 'dev')
- atm_remapped: float32 [4, 8, 12, 1024], P('grp', 'dev')
The draws below stay inside these ranges and needn't reach their ends.
Inputs may be any that keep to these rules, and one draw needn't show every extreme that they name: `margin_counts`: the 1024 counts of one partition sum to 1536, and one of them equals 4. `block_owner`: no partition sends more than 12 of its 12 blocks to one ocean group, and every partition sends exactly 12 blocks to one of them.
All inputs are finite; a program needn't handle non-finite values.
Results may differ from the reference program's by a relative error of at most 0.0029.
Values may be sent and summed in bfloat16 or wider, within the bound.
A program may use at most 64 MiB of HBM per device.

```python
import math
import jax
import jax.numpy as jnp
import numpy as np
from jax import lax

LEV_A = 128
LEV_O = 80
FLUX = 24
RET = 12
KA = 4
KO = 6
BLOCK = 128
HS = 128
COLS = 1024
CELLS = 2048
ROWS = 1536
NB = 12
ATM_GRPS = 2
OCN_GRPS = 2
CAP = 12
N_GRP = 4
N_DEV = 8


def draw_block_owner(key, part):
    first_key, second_key = jax.random.split(jax.random.fold_in(key, 7311))
    partitions = N_GRP * N_DEV
    orders = jax.vmap(lambda k: jax.random.permutation(k, OCN_GRPS))(jax.random.split(first_key, partitions))
    listed = jnp.repeat(orders, CAP, axis=1)[:, :NB]
    shuffled = jax.vmap(lambda k, row: jax.random.permutation(k, row))(jax.random.split(second_key, partitions), listed)
    return shuffled.reshape(N_GRP, N_DEV, NB, 1).astype(jnp.int32)


def with_ends(array, key, least, top_value):
    spot = [jax.random.randint(jax.random.fold_in(key, axis), (), 0, length) for axis, length in enumerate(array.shape)]
    widest = array.shape.index(max(array.shape))
    next_to = spot[:widest] + [(spot[widest] + 1) % array.shape[widest]] + spot[widest + 1:]
    return array.at[tuple(spot)].set(least).at[tuple(next_to)].set(top_value)


def block_scale(own_key, dims, pieces, low, largest):
    factor_of = 1.0
    for position, parts in pieces:
        draws = jax.random.uniform(jax.random.fold_in(jax.random.fold_in(own_key, 6), position), (parts,), jnp.float32, low / len(pieces), largest / len(pieces))
        factor_of = factor_of * jnp.repeat(jnp.exp(draws), dims[position] // parts).reshape((-1,) + (1,) * (len(dims) - 1 - position))
    return factor_of


def length_profile(amount, total, most, slope):
    weights = [(1 << 20) // math.isqrt(standing ** slope) + 1 for standing in range(2, amount + 1)]
    spare, given = total - most - (amount - 1), [1] * (amount - 1)
    while spare > 0:
        candidates = [i for i in range(amount - 1) if given[i] < most]
        whole, left = sum([weights[i] for i in candidates]), spare
        for i in candidates:
            addition = min(most - given[i], max(1, left * weights[i] // whole), spare)
            given[i] = given[i] + addition
            spare = spare - addition
    return np.array([most] + given)


def ragged(stream_key, number_of, total, reach, skew):
    if number_of == 2:
        one = jax.random.randint(stream_key, (), max(1, total - reach), min(reach, total - 1) + 1)
        return jnp.stack([one, total - one])
    sizes = jnp.asarray(length_profile(number_of, total, reach, skew), jnp.int32)
    couples = (number_of - 1) // 2
    source_of, sink = sizes[1:1 + 2 * couples:2], sizes[2:2 + 2 * couples:2]
    slack = jnp.minimum(source_of - 1, reach - sink)
    passed = jax.random.randint(jax.random.fold_in(stream_key, 1), (couples,), 0, 1 << 20) % (slack + 1)
    sizes = sizes.at[1:1 + 2 * couples:2].set(source_of - passed).at[2:2 + 2 * couples:2].set(sink + passed)
    return sizes[jax.random.permutation(jax.random.fold_in(stream_key, 2), number_of)]


def bell_draw(rng, dims, deviation, most, pieces=(), held_as=jnp.bfloat16):
    drawn = deviation * jax.random.normal(rng, dims, jnp.float32)
    if pieces:
        drawn = drawn * block_scale(rng, dims, pieces, -0.22, 0.18)
    return jnp.clip(drawn, -most, most).astype(held_as)


def setup_inputs(seed: int = 0) -> dict:
    key_of = jax.random.split(jax.random.key(seed), 16)
    return {
        "atm_state": bell_draw(key_of[0], (N_GRP, N_DEV, LEV_A, COLS), 1.0, 6.0, ((0, 4), (1, 8)), jnp.float32),
        "atm_nbrs": with_ends(jax.random.randint(key_of[1], (N_GRP, N_DEV, KA, COLS), 0, COLS + 2 * HS), jax.random.fold_in(key_of[1], 1), 0, (COLS + 2 * HS) - 1).astype(jnp.int32),
        "atm_send": with_ends(jax.random.randint(key_of[2], (N_GRP, N_DEV, 2 * HS), 0, COLS), jax.random.fold_in(key_of[2], 1), 0, COLS - 1).astype(jnp.int32),
        "atm_mix": jnp.clip(0.2 + 0.400000021 * jax.random.uniform(key_of[3], (N_GRP, N_DEV, COLS), jnp.float32) ** block_scale(key_of[3], (N_GRP, N_DEV, COLS), ((0, 4), (1, 8)), -0.2, 0.2), 0.2, 0.6),
        "flux_weight": bell_draw(key_of[4], (FLUX, LEV_A), LEV_A ** -0.5, 0.5, (), jnp.float32),
        "margin_counts": jax.vmap(lambda own: ragged(own, COLS, ROWS, 4, 1))(jax.random.split(key_of[5], N_GRP * N_DEV)).reshape((N_GRP, N_DEV, COLS)).astype(jnp.int32),
        "margin_weight": jnp.clip(jnp.exp(math.log(1.0) - 2.9957323 * jax.random.uniform(key_of[6], (N_GRP, N_DEV, ROWS), jnp.float32) ** block_scale(key_of[6], (N_GRP, N_DEV, ROWS), ((0, 4), (1, 8)), -0.2, 0.2)), 0.05, 1.0),
        "block_owner": draw_block_owner(jax.random.fold_in(key_of[15], 71), 0),
        "recv_cols": with_ends(jax.random.randint(key_of[8], (N_GRP, N_DEV, ATM_GRPS, CAP, BLOCK), 0, CELLS), jax.random.fold_in(key_of[8], 1), 0, CELLS - 1).astype(jnp.int32),
        "ocn_state": bell_draw(key_of[9], (N_GRP, N_DEV, LEV_O, CELLS), 1.0, 6.0, ((0, 4), (1, 8)), jnp.float32),
        "ocn_nbrs": with_ends(jax.random.randint(key_of[10], (N_GRP, N_DEV, KO, CELLS), 0, CELLS + 2 * HS), jax.random.fold_in(key_of[10], 1), 0, (CELLS + 2 * HS) - 1).astype(jnp.int32),
        "ocn_send": with_ends(jax.random.randint(key_of[11], (N_GRP, N_DEV, 2 * HS), 0, CELLS), jax.random.fold_in(key_of[11], 1), 0, CELLS - 1).astype(jnp.int32),
        "ocn_mix": jnp.clip(0.1 + 0.3 * jax.random.uniform(key_of[12], (N_GRP, N_DEV, CELLS), jnp.float32) ** block_scale(key_of[12], (N_GRP, N_DEV, CELLS), ((0, 4), (1, 8)), -0.2, 0.2), 0.1, 0.4),
        "force_weight": bell_draw(key_of[13], (LEV_O, FLUX), FLUX ** -0.5, 1.25, (), jnp.float32),
        "ret_weight": bell_draw(key_of[14], (RET, LEV_O), LEV_O ** -0.5, 0.625, (), jnp.float32),
    }


EXACT_DOT = lax.Precision.HIGHEST


def stencil(state, pool, neighbours, mixing):
    total = jnp.take(pool, neighbours[0], axis=1)
    for which in range(1, neighbours.shape[0]):
        total = total + jnp.take(pool, neighbours[which], axis=1)
    return state + mixing[None, :] * (total / neighbours.shape[0] - state)


def pick_columns(values, indices):
    return jnp.take(values, indices, axis=1)


def pooled(state, send_list):
    half = send_list.shape[-1] // 2
    packed = jax.vmap(jax.vmap(pick_columns))(state, send_list)
    from_lower = jnp.roll(packed[..., half:], 1, axis=1)
    from_upper = jnp.roll(packed[..., :half], -1, axis=1)
    return jnp.concatenate([state, from_lower, from_upper], axis=3)


def column_ids(counts):
    return jnp.repeat(jnp.arange(COLS, dtype=jnp.int32), counts, total_repeat_length=ROWS)


def block_slots(owner):
    order = jnp.arange(owner.shape[0], dtype=jnp.int32)
    earlier = (owner[None, :] == owner[:, None]) & (order[None, :] < order[:, None])
    return jnp.sum(earlier.astype(jnp.int32), axis=1)


def remap_back(values, weights, column):
    weighted = jax.ops.segment_sum(values * weights[:, None], column, num_segments=COLS)
    weight_sum = jax.ops.segment_sum(weights, column, num_segments=COLS)
    return (weighted / weight_sum[:, None]).T


def reference(atm_state, atm_nbrs, atm_send, atm_mix, flux_weight, margin_counts, margin_weight, block_owner, recv_cols, ocn_state, ocn_nbrs, ocn_send, ocn_mix, force_weight, ret_weight):
    groups = atm_state.shape[0]
    devices = atm_state.shape[1]
    atm_groups = groups // 2
    sweep = jax.vmap(jax.vmap(stencil))
    air = atm_state[:atm_groups]
    air_next = sweep(air, pooled(air, atm_send[:atm_groups]), atm_nbrs[:atm_groups], atm_mix[:atm_groups])
    atm_next = jnp.concatenate([air_next, atm_state[atm_groups:]], axis=0)
    sea = ocn_state[atm_groups:]
    sea_base = sweep(sea, pooled(sea, ocn_send[atm_groups:]), ocn_nbrs[atm_groups:], ocn_mix[atm_groups:])
    fluxes = jnp.einsum("fl,gdlc->gdfc", flux_weight, air_next, precision=EXACT_DOT)
    column = jax.vmap(jax.vmap(column_ids))(margin_counts[:atm_groups])
    weights = margin_weight[:atm_groups]
    row_values = (jax.vmap(jax.vmap(pick_columns))(fluxes, column) * weights[:, :, None, :]).astype(jnp.bfloat16)
    owner = block_owner[:atm_groups, :, :, 0]
    slot = jax.vmap(jax.vmap(block_slots))(owner)
    sender = jnp.arange(atm_groups, dtype=jnp.int32)[:, None, None]
    partition = jnp.arange(devices, dtype=jnp.int32)[None, :, None]
    cell = recv_cols[atm_groups + owner, partition, sender, slot]
    target = ((owner * devices + partition)[..., None] * CELLS + cell).reshape(-1)
    flat_rows = row_values.reshape(atm_groups, devices, FLUX, NB, BLOCK).transpose(0, 1, 3, 4, 2).reshape(-1, FLUX).astype(jnp.float32)
    cell_flux = jnp.zeros((OCN_GRPS * devices * CELLS, FLUX), jnp.float32).at[target].add(flat_rows)
    cell_flux = cell_flux.reshape(OCN_GRPS, devices, CELLS, FLUX)
    forcing = jnp.einsum("lf,odcf->odlc", force_weight, cell_flux, precision=EXACT_DOT)
    ocn_next = jnp.concatenate([ocn_state[:atm_groups], sea_base + forcing], axis=0)
    returned = jnp.einsum("rl,odlc->odcr", ret_weight, sea, precision=EXACT_DOT).astype(jnp.bfloat16)
    looked = returned.reshape(-1, RET)[target].astype(jnp.float32).reshape(atm_groups, devices, ROWS, RET)
    remapped = jax.vmap(jax.vmap(remap_back))(looked, weights, column)
    remapped = jnp.concatenate([remapped, jnp.zeros((groups - atm_groups, devices, RET, COLS), jnp.float32)], axis=0)
    return atm_next, ocn_next, remapped
```

```python
import functools

import jax
import jax.numpy as jnp
from jax import lax
from jax.experimental import pallas as pl
from jax.experimental.pallas import tpu as pltpu
from jax.sharding import PartitionSpec as P

EXACT = lax.Precision.HIGHEST
BF = jnp.bfloat16
F32 = jnp.float32
NT = (((1,), (1,)), ((), ()))


def split(x):
    hi = x.astype(BF)
    return hi, (x - hi.astype(F32)).astype(BF)


def mm(a, b):
    return jnp.dot(a, b, preferred_element_type=F32)


def one_hot(idx, rows, base):
    width = idx.shape[1]
    place = lax.broadcasted_iota(jnp.int32, (rows, width), 0) + base
    return jnp.where(place == idx, 1.0, 0.0).astype(BF)


def counts_matrix(out_ref, high_ref, idx_rows, base, at):
    width = idx_rows[0].shape[1]
    highs = out_ref.shape[0] // base
    bits = base.bit_length() - 1
    low = [i & (base - 1) for i in idx_rows]
    for k, i in enumerate(idx_rows):
        high = jnp.broadcast_to(i >> bits, (16, width))
        for h in range(highs):
            high_ref[k * highs + h, :, :width] = jnp.where(high == h, 1.0, 0.0).astype(BF)
    for t in range(base // 16):
        parts = [one_hot(i, 16, t * 16) for i in low]
        for h in range(highs):
            total = parts[0] * high_ref[h, :, :width]
            for k in range(1, len(parts)):
                total = total + parts[k] * high_ref[k * highs + h, :, :width]
            out_ref[pl.ds(h * base + t * 16, 16), at] = total


def base_of(length):
    return 256 if length % 256 == 0 else 128


def kernel(
    sizes,
    air_ref, anbr_ref, asend_ref, amix_ref, fw_ref, counts_ref, mw_ref, owner_ref,
    recv_ref, sea_ref, onbr_ref, osend_ref, omix_ref, force_ref, retw_ref,
    air_out, sea_out, back_out,
    pack, halo, apool, opool, amat, omat, member, cellmat, high,
    rows, up_out, up_in, down_out, down_in, retw, slab, ret_bf,
    halo_send, halo_recv, x_send, x_recv,
):
    groups, devs, air_groups = sizes
    sea_groups = groups - air_groups
    g, d = lax.axis_index("grp"), lax.axis_index("dev")
    lower, upper = lax.rem(d + devs - 1, devs), lax.rem(d + 1, devs)
    is_air = g < air_groups
    half = halo.shape[2]
    capacity, block = recv_ref.shape[3], recv_ref.shape[4]
    span = capacity * block
    levels_a, columns = air_ref.shape[2:]
    levels_o, cells = sea_ref.shape[2:]
    fields = fw_ref.shape[0]
    ret_fields = retw_ref.shape[0]
    ret_pad = retw.shape[0]
    blocks = owner_ref.shape[2]
    first = jnp.where(is_air, air_groups, 0)
    mine = jnp.where(is_air, g, g - air_groups)
    partners = air_groups

    barrier = pltpu.get_barrier_semaphore()
    pl.semaphore_signal(barrier, inc=1, device_id={"dev": lower})
    pl.semaphore_signal(barrier, inc=1, device_id={"dev": upper})
    for p in range(partners):
        pl.semaphore_signal(barrier, inc=1, device_id={"grp": first + p})

    def packed(state_ref, send_ref, pool):
        levels, length = state_ref.shape[2:]
        top, rest = split(state_ref[0, 0])
        pool[:levels, :length] = top
        pool[levels:, :length] = rest
        picker = one_hot(send_ref[0], length, 0)
        chosen = mm(top, picker).astype(BF)
        pack[0, :levels, :] = chosen[:, :half]
        pack[1, :levels, :] = chosen[:, half:]
        if levels < pack.shape[1]:
            pack[:, levels:, :] = jnp.zeros((2, pack.shape[1] - levels, half), BF)

    @pl.when(is_air)
    def _():
        packed(air_ref, asend_ref, apool)

    @pl.when(jnp.logical_not(is_air))
    def _():
        packed(sea_ref, osend_ref, opool)

    pl.semaphore_wait(barrier, 2 + partners)
    to_upper = pltpu.make_async_remote_copy(
        src_ref=pack.at[1], dst_ref=halo.at[0], send_sem=halo_send.at[0],
        recv_sem=halo_recv.at[0], device_id={"dev": upper})
    to_lower = pltpu.make_async_remote_copy(
        src_ref=pack.at[0], dst_ref=halo.at[1], send_sem=halo_send.at[1],
        recv_sem=halo_recv.at[1], device_id={"dev": lower})
    to_upper.start()
    to_lower.start()

    up = [
        pltpu.make_async_remote_copy(
            src_ref=up_out.at[p], dst_ref=up_in.at[mine], send_sem=x_send.at[p],
            recv_sem=x_recv.at[mine], device_id={"grp": first + p})
        for p in range(partners)
    ]
    down = [
        pltpu.make_async_remote_copy(
            src_ref=down_out.at[p], dst_ref=down_in.at[mine], send_sem=x_send.at[p],
            recv_sem=x_recv.at[mine], device_id={"grp": first + p})
        for p in range(partners)
    ]

    def take_halo(pool, levels, length):
        to_upper.wait()
        to_lower.wait()
        for side in range(2):
            at = slice(length + side * half, length + (side + 1) * half)
            pool[:levels, at] = halo[side, :levels, :]
            pool[levels:, at] = jnp.zeros((levels, half), BF)

    @pl.when(is_air)
    def _():
        sea_out[0, 0] = sea_ref[0, 0]
        neighbours = anbr_ref.shape[2]
        base = base_of(amat.shape[0])
        width = high.shape[2]

        def build(c, _):
            at = pl.ds(pl.multiple_of(c * width, width), width)
            rows_in = [anbr_ref[0, 0, k : k + 1, at] for k in range(neighbours)]
            counts_matrix(amat, high, rows_in, base, at)
            return _

        lax.fori_loop(0, columns // width, build, 0)

        cnt = jnp.broadcast_to(counts_ref[0].astype(F32), (128, columns)).astype(BF)
        row_count = mw_ref.shape[2]

        def build_member(c, _):
            shape = (128, columns)
            a = lax.broadcasted_iota(jnp.int32, shape, 0) + c * 128
            b = lax.broadcasted_iota(jnp.int32, shape, 1)
            upto = jnp.where(b <= a, 1.0, 0.0).astype(BF)
            before = jnp.where(b < a, 1.0, 0.0).astype(BF)
            end = lax.dot_general(upto, cnt, NT, preferred_element_type=F32)
            start = lax.dot_general(before, cnt, NT, preferred_element_type=F32)
            for r in range(row_count // 128):
                at = lax.broadcasted_iota(jnp.int32, (128, 128), 1).astype(F32) + r * 128.0
                inside = (at >= start) & (at < end)
                member[pl.ds(pl.multiple_of(c * 128, 128), 128), r * 128 : (r + 1) * 128] = (
                    jnp.where(inside, 1.0, 0.0).astype(BF))
            return _

        lax.fori_loop(0, columns // 128, build_member, 0)
        take_halo(apool, levels_a, columns)

        def sweep(c, _):
            at = pl.ds(pl.multiple_of(c * width, width), width)
            both = mm(apool[...], amat[:, at])
            mean = (both[:levels_a] + both[levels_a:]) * (1.0 / neighbours)
            state = air_ref[0, 0, :, at]
            new = state + amix_ref[0, :, at] * (mean - state)
            air_out[0, 0, :, at] = new
            flux = jnp.dot(fw_ref[...], new, precision=EXACT, preferred_element_type=F32)
            top, rest = split(flux)
            slab[:fields, at] = top
            slab[fields : 2 * fields, at] = rest
            return _

        lax.fori_loop(0, columns // width, sweep, 0)
        for b in range(blocks):
            at = slice(b * block, (b + 1) * block)
            both = mm(slab[: 2 * fields, :columns], member[:, at])
            weight = mw_ref[0, :, at]
            rows[b] = (both[:fields] + both[fields:]) * weight
        owner = [owner_ref[0, 0, b, 0] for b in range(blocks)]
        slot = []
        for b in range(blocks):
            s = jnp.int32(0)
            for e in range(b):
                s = s + jnp.where(owner[e] == owner[b], 1, 0)
            slot.append(s)
        place = [owner[b] * capacity + slot[b] for b in range(blocks)]
        for o in range(sea_groups):
            for k in range(capacity):
                source = jnp.int32(0)
                valid = jnp.int32(0)
                for b in range(blocks):
                    hit = place[b] == o * capacity + k
                    source = jnp.where(hit, b, source)
                    valid = jnp.where(hit, 1, valid)
                value = rows[source] * valid.astype(F32)
                up_out[o, :, k * block : (k + 1) * block] = value.astype(BF)
            up[o].start()
        for p in range(partners):
            pltpu.make_async_remote_copy(
                src_ref=down_out.at[p], dst_ref=down_in.at[p], send_sem=x_send.at[p],
                recv_sem=x_recv.at[p], device_id={"grp": first + p}).wait_recv()
        for b in range(blocks):
            at = slice(b * block, (b + 1) * block)
            weight = jnp.broadcast_to(mw_ref[0, :, at], (ret_pad, block))
            value = down_in[owner[b], slot[b]].astype(F32) * weight
            top, rest = split(value)
            wtop, wrest = split(weight)
            for i, part in enumerate((top, rest, wtop, wrest)):
                slab[i * ret_pad : (i + 1) * ret_pad, at] = part
        depth = 4 * ret_pad
        r0 = lax.broadcasted_iota(jnp.int32, (2 * ret_pad, depth), 0)
        c0 = lax.broadcasted_iota(jnp.int32, (2 * ret_pad, depth), 1)
        near = jnp.where(r0 < ret_pad, r0, r0 + ret_pad)
        pick = jnp.where((c0 == near) | (c0 == near + ret_pad), 1.0, 0.0)

        sums = lax.dot_general(
            member[...], slab[:depth, :row_count], NT, preferred_element_type=F32)
        both = lax.dot_general(pick, sums, NT, precision=EXACT, preferred_element_type=F32)
        back_out[0, 0] = (both[:ret_pad] / both[ret_pad:])[:ret_fields]
        for p in range(partners):
            up[p].wait_send()

    @pl.when(jnp.logical_not(is_air))
    def _():
        air_out[0, 0] = air_ref[0, 0]
        back_out[0, 0] = jnp.zeros(back_out.shape[2:], F32)
        neighbours = onbr_ref.shape[2]
        width = high.shape[2]
        retw[...] = jnp.zeros(retw.shape, F32)
        retw[:ret_fields] = retw_ref[...]
        ret_bf[...] = jnp.dot(
            retw[...], sea_ref[0, 0], precision=EXACT, preferred_element_type=F32).astype(BF)
        base = base_of(cells)
        for s in range(air_groups):

            def build(k, _):
                at = pl.ds(pl.multiple_of(s * span + k * 2 * block, 2 * block), 2 * block)
                idx = jnp.concatenate(
                    [recv_ref[0, 0, s, pl.ds(2 * k + i, 1), :] for i in range(2)], axis=1)
                counts_matrix(cellmat, high, [idx], base, at)
                looked = mm(ret_bf[...], cellmat[:, at]).astype(BF)
                for i in range(2):
                    down_out[s, 2 * k + i] = looked[:, i * block : (i + 1) * block]
                return _

            lax.fori_loop(0, capacity // 2, build, 0)
            down[s].start()
        take_halo(opool, levels_o, cells)
        base_p = base_of(omat.shape[0])

        def sweep(c, _):
            at = pl.ds(pl.multiple_of(c * width, width), width)
            rows_in = [onbr_ref[0, 0, k : k + 1, at] for k in range(neighbours)]
            counts_matrix(omat, high, rows_in, base_p, slice(0, width))
            both = mm(opool[...], omat[...])
            mean = (both[:levels_o] + both[levels_o:]) * (1.0 / neighbours)
            state = sea_ref[0, 0, :, at]
            sea_out[0, 0, :, at] = state + omix_ref[0, :, at] * (mean - state)
            return _

        lax.fori_loop(0, cells // width, sweep, 0)
        for p in range(partners):
            pltpu.make_async_remote_copy(
                src_ref=up_out.at[p], dst_ref=up_in.at[p], send_sem=x_send.at[p],
                recv_sem=x_recv.at[p], device_id={"grp": first + p}).wait_recv()
        tall = min(cells, 512)

        def force(c, _):
            at = pl.ds(pl.multiple_of(c * tall, tall), tall)
            flux = jnp.zeros((tall, fields), F32)
            for s in range(air_groups):
                flux = flux + lax.dot_general(
                    cellmat[at, s * span : (s + 1) * span], up_in[s], NT,
                    preferred_element_type=F32)
            sea_out[0, 0, :, at] += lax.dot_general(
                force_ref[...], flux, NT, precision=EXACT, preferred_element_type=F32)
            return _

        lax.fori_loop(0, cells // tall, force, 0)
        for p in range(partners):
            down[p].wait_send()


def solution(mesh):
    groups, devs = mesh.shape["grp"], mesh.shape["dev"]
    in_specs = (
        P("grp", "dev", None, None), P("grp", "dev", None, None), P("grp", "dev", None),
        P("grp", "dev", None), P(), P("grp", "dev", None), P("grp", "dev", None),
        P("grp", "dev", None, None), P("grp", "dev", None, None, None),
        P("grp", "dev", None, None), P("grp", "dev", None, None), P("grp", "dev", None),
        P("grp", "dev", None), P(), P(),
    )
    out_specs = (P("grp", "dev", None, None),) * 3

    def on_device(*args):
        air, anbr, asend, _, fw, _, mw, owner, recv, sea, onbr, _, _, _, ret = args
        levels_a, columns = air.shape[2:]
        levels_o, cells = sea.shape[2:]
        half = asend.shape[2] // 2
        air_groups, capacity, block = recv.shape[2:]
        sea_groups = groups - air_groups
        fields, ret_fields = fw.shape[0], ret.shape[0]
        ret_pad = -(-ret_fields // 16) * 16
        row_count = mw.shape[2]
        pool_a, pool_o = columns + 2 * half, cells + 2 * half
        width = 256
        deep = max(
            anbr.shape[2] * (pool_a // base_of(pool_a)),
            onbr.shape[2] * (pool_o // base_of(pool_o)),
            cells // base_of(cells),
        )
        vmem = pl.BlockSpec(memory_space=pltpu.VMEM)
        smem = pl.BlockSpec(memory_space=pltpu.SMEM)
        ins = [vmem] * 15
        ins[7] = smem
        levels = max(levels_a, levels_o)
        V = pltpu.VMEM
        scratch = [
            V((2, levels, half), BF), V((2, levels, half), BF),
            V((2 * levels_a, pool_a), BF), V((2 * levels_o, pool_o), BF),
            V((pool_a, columns), BF), V((pool_o, width), BF),
            V((columns, row_count), BF), V((cells, air_groups * capacity * block), BF),
            V((deep, 16, width), BF),
            V((owner.shape[2], fields, block), F32),
            V((sea_groups, fields, capacity * block), BF),
            V((air_groups, fields, capacity * block), BF),
            V((air_groups, capacity, ret_pad, block), BF),
            V((sea_groups, capacity, ret_pad, block), BF),
            V((ret_pad, levels_o), F32),
            V((max(4 * ret_pad, 2 * fields), max(row_count, columns)), BF),
            V((ret_pad, cells), BF),
            pltpu.SemaphoreType.DMA((2,)), pltpu.SemaphoreType.DMA((2,)),
            pltpu.SemaphoreType.DMA((air_groups,)), pltpu.SemaphoreType.DMA((air_groups,)),
        ]
        return pl.pallas_call(
            functools.partial(kernel, (groups, devs, air_groups)),
            out_shape=(
                jax.ShapeDtypeStruct(air.shape, F32),
                jax.ShapeDtypeStruct(sea.shape, F32),
                jax.ShapeDtypeStruct((1, 1, ret_fields, columns), F32),
            ),
            in_specs=ins,
            out_specs=(vmem,) * 3,
            scratch_shapes=scratch,
            compiler_params=pltpu.CompilerParams(
                collective_id=0, has_side_effects=True, vmem_limit_bytes=60 * 1024 * 1024),
            name="couple",
        )(*args)

    return jax.shard_map(
        on_device, mesh=mesh, in_specs=in_specs, out_specs=out_specs, check_vma=False)
```

```python
import functools

import jax
import jax.numpy as jnp
from jax import lax
from jax.experimental import pallas as pl
from jax.experimental.pallas import tpu as pltpu
from jax.sharding import PartitionSpec as P

EXACT = lax.Precision.HIGHEST
BF = jnp.bfloat16
F32 = jnp.float32
NT = (((1,), (1,)), ((), ()))


def split(x):
    hi = x.astype(BF)
    return hi, (x - hi.astype(F32)).astype(BF)


def mm(a, b):
    return jnp.dot(a, b, preferred_element_type=F32)


def low_hot(low, t):
    place = lax.broadcasted_iota(jnp.int32, low.shape, 0).astype(F32).astype(BF)
    return jnp.where(low - jnp.asarray(16.0 * t, BF) == place, jnp.asarray(1, BF), jnp.asarray(0, BF))


def as_rows(idx, rows):
    return jnp.broadcast_to(idx.astype(F32), (rows, idx.shape[1])).astype(BF)


def one_hot(idx, rows, base):
    width = idx.shape[1]
    place = lax.broadcasted_iota(jnp.int32, (rows, width), 0) + base
    return jnp.where(place == idx, 1.0, 0.0).astype(BF)


def counts_matrix(out_ref, high_ref, idx_rows, base, at):
    width = idx_rows[0].shape[1]
    highs = out_ref.shape[0] // base
    bits = base.bit_length() - 1
    low = [as_rows(i & (base - 1), 16) for i in idx_rows]
    for k, i in enumerate(idx_rows):
        high = jnp.broadcast_to(i >> bits, (16, width))
        for h in range(highs):
            high_ref[k * highs + h, :, :width] = jnp.where(high == h, 1.0, 0.0).astype(BF)
    for t in range(base // 16):
        parts = [low_hot(i, t) for i in low]
        for h in range(highs):
            total = parts[0] * high_ref[h, :, :width]
            for k in range(1, len(parts)):
                total = total + parts[k] * high_ref[k * highs + h, :, :width]
            out_ref[pl.ds(h * base + t * 16, 16), at] = total


def base_of(length):
    return 256 if length % 256 == 0 else 128


def kernel(
    sizes,
    air_ref, anbr_ref, asend_ref, amix_ref, fw_ref, counts_ref, mw_ref, owner_ref,
    recv_ref, sea_ref, onbr_ref, osend_ref, omix_ref, force_ref, retw_ref,
    air_out, sea_out, back_out,
    pack, halo, apool, opool, amat, omat0, omat1, member, lowmat, spread, high, high1,
    rows, up_out, up_in, down_out, down_in, retw, slab, ret_bf,
    halo_send, halo_recv, x_send, x_recv,
):
    groups, devs, air_groups = sizes
    sea_groups = groups - air_groups
    g, d = lax.axis_index("grp"), lax.axis_index("dev")
    lower, upper = lax.rem(d + devs - 1, devs), lax.rem(d + 1, devs)
    is_air = g < air_groups
    half = halo.shape[2]
    capacity, block = recv_ref.shape[2], recv_ref.shape[4]
    span = capacity * block
    levels_a, columns = air_ref.shape[2:]
    levels_o, cells = sea_ref.shape[2:]
    fields = fw_ref.shape[0]
    field_pad = spread.shape[0] // (cells // lowmat.shape[0])
    ret_fields = retw_ref.shape[0]
    ret_pad = retw.shape[0]
    blocks = owner_ref.shape[3]
    first = jnp.where(is_air, air_groups, 0)
    mine = jnp.where(is_air, g, g - air_groups)
    partners = air_groups

    barrier = pltpu.get_barrier_semaphore()
    pl.semaphore_signal(barrier, inc=1, device_id={"dev": lower})
    pl.semaphore_signal(barrier, inc=1, device_id={"dev": upper})
    for p in range(partners):
        pl.semaphore_signal(barrier, inc=1, device_id={"grp": first + p})

    def packed(state_ref, send_ref, pool):
        levels, length = state_ref.shape[2:]
        top = state_ref[0, 0].astype(BF)
        pool[:, :length] = top
        picker = one_hot(send_ref[0], length, 0)
        chosen = mm(top, picker).astype(BF)
        pack[0, :levels, :] = chosen[:, :half]
        pack[1, :levels, :] = chosen[:, half:]
        if levels < pack.shape[1]:
            pack[:, levels:, :] = jnp.zeros((2, pack.shape[1] - levels, half), BF)

    @pl.when(is_air)
    def _():
        packed(air_ref, asend_ref, apool)

    @pl.when(jnp.logical_not(is_air))
    def _():
        packed(sea_ref, osend_ref, opool)

    pl.semaphore_wait(barrier, 2 + partners)
    to_upper = pltpu.make_async_remote_copy(
        src_ref=pack.at[1], dst_ref=halo.at[0], send_sem=halo_send.at[0],
        recv_sem=halo_recv.at[0], device_id={"dev": upper})
    to_lower = pltpu.make_async_remote_copy(
        src_ref=pack.at[0], dst_ref=halo.at[1], send_sem=halo_send.at[1],
        recv_sem=halo_recv.at[1], device_id={"dev": lower})
    to_upper.start()
    to_lower.start()

    up = [
        pltpu.make_async_remote_copy(
            src_ref=up_out.at[p], dst_ref=up_in.at[mine], send_sem=x_send.at[p],
            recv_sem=x_recv.at[mine], device_id={"grp": first + p})
        for p in range(partners)
    ]
    down = [
        pltpu.make_async_remote_copy(
            src_ref=down_out.at[p], dst_ref=down_in.at[mine], send_sem=x_send.at[p],
            recv_sem=x_recv.at[mine], device_id={"grp": first + p})
        for p in range(partners)
    ]

    def take_halo(pool, levels, length):
        to_upper.wait()
        to_lower.wait()
        for side in range(2):
            at = slice(length + side * half, length + (side + 1) * half)
            pool[:, at] = halo[side, :levels, :]

    @pl.when(is_air)
    def _():
        sea_out[0, 0] = sea_ref[0, 0]
        neighbours = anbr_ref.shape[2]
        base = base_of(amat.shape[0])
        width = high.shape[2]

        def build(c, _):
            at = pl.ds(pl.multiple_of(c * width, width), width)
            rows_in = [anbr_ref[0, 0, k : k + 1, at] for k in range(neighbours)]
            counts_matrix(amat, high, rows_in, base, at)
            return _

        lax.fori_loop(0, columns // width, build, 0)

        cnt = jnp.broadcast_to(counts_ref[0].astype(F32), (128, columns)).astype(BF)
        row_count = mw_ref.shape[2]

        def build_member(c, _):
            shape = (128, columns)
            a = lax.broadcasted_iota(jnp.int32, shape, 0) + c * 128
            b = lax.broadcasted_iota(jnp.int32, shape, 1)
            upto = jnp.where(b <= a, 1.0, 0.0).astype(BF)
            before = jnp.where(b < a, 1.0, 0.0).astype(BF)
            end = lax.dot_general(upto, cnt, NT, preferred_element_type=F32)
            start = lax.dot_general(before, cnt, NT, preferred_element_type=F32)
            for r in range(row_count // 128):
                at = lax.broadcasted_iota(jnp.int32, (128, 128), 1).astype(F32) + r * 128.0
                inside = (at >= start) & (at < end)
                member[pl.ds(pl.multiple_of(c * 128, 128), 128), r * 128 : (r + 1) * 128] = (
                    jnp.where(inside, 1.0, 0.0).astype(BF))
            return _

        lax.fori_loop(0, columns // 128, build_member, 0)
        take_halo(apool, levels_a, columns)

        for c in range(columns // width):
            at = slice(c * width, (c + 1) * width)
            mean = mm(apool[...], amat[:, at]) * (1.0 / neighbours)
            state = air_ref[0, 0, :, at]
            new = state + amix_ref[0, :, at] * (mean - state)
            air_out[0, 0, :, at] = new
            flux = jnp.dot(fw_ref[...], new, precision=EXACT, preferred_element_type=F32)
            top, rest = split(flux)
            slab[:fields, at] = top
            slab[fields : 2 * fields, at] = rest
        both = mm(slab[: 2 * fields, :columns], member[...])
        values = (both[:fields] + both[fields:]) * mw_ref[0]
        for b in range(blocks):
            rows[b] = values[:, b * block : (b + 1) * block]
        owner = [owner_ref[0, 0, 0, b] for b in range(blocks)]
        slot = []
        for b in range(blocks):
            s = jnp.int32(0)
            for e in range(b):
                s = s + jnp.where(owner[e] == owner[b], 1, 0)
            slot.append(s)
        place = [owner[b] * capacity + slot[b] for b in range(blocks)]
        for o in range(sea_groups):
            for k in range(capacity):
                source = jnp.int32(0)
                valid = jnp.int32(0)
                for b in range(blocks):
                    hit = place[b] == o * capacity + k
                    source = jnp.where(hit, b, source)
                    valid = jnp.where(hit, 1, valid)
                value = rows[source] * valid.astype(F32)
                up_out[o, :, k * block : (k + 1) * block] = value.astype(BF)
            up[o].start()
        for p in range(partners):
            pltpu.make_async_remote_copy(
                src_ref=down_out.at[p], dst_ref=down_in.at[p], send_sem=x_send.at[p],
                recv_sem=x_recv.at[p], device_id={"grp": first + p}).wait_recv()
        for b in range(blocks):
            at = slice(b * block, (b + 1) * block)
            weight = jnp.broadcast_to(mw_ref[0, :, at], (ret_pad, block))
            value = down_in[owner[b], slot[b]].astype(F32) * weight
            top, rest = split(value)
            wtop, wrest = split(weight)
            for i, part in enumerate((top, rest, wtop, wrest)):
                slab[i * ret_pad : (i + 1) * ret_pad, at] = part
        depth = 4 * ret_pad
        r0 = lax.broadcasted_iota(jnp.int32, (2 * ret_pad, depth), 0)
        c0 = lax.broadcasted_iota(jnp.int32, (2 * ret_pad, depth), 1)
        near = jnp.where(r0 < ret_pad, r0, r0 + ret_pad)
        pick = jnp.where((c0 == near) | (c0 == near + ret_pad), 1.0, 0.0)

        sums = lax.dot_general(
            member[...], slab[:depth, :row_count], NT, preferred_element_type=F32)
        both = lax.dot_general(pick, sums, NT, precision=EXACT, preferred_element_type=F32)
        ratio = both[:ret_pad] / both[ret_pad:]
        for f in range(ret_fields):
            back_out[0, f] = ratio[f : f + 1]
        for p in range(partners):
            up[p].wait_send()

    @pl.when(jnp.logical_not(is_air))
    def _():
        air_out[0, 0] = air_ref[0, 0]
        back_out[...] = jnp.zeros(back_out.shape, F32)
        neighbours = onbr_ref.shape[1]
        width = high.shape[2]
        base = lowmat.shape[0]
        bits = base.bit_length() - 1
        highs = cells // base
        retw[...] = jnp.zeros(retw.shape, F32)
        retw[:ret_fields] = retw_ref[...]
        returned = jnp.dot(
            retw[...], sea_ref[0, 0], precision=EXACT, preferred_element_type=F32).astype(BF)
        for h in range(highs):
            ret_bf[h * ret_pad : (h + 1) * ret_pad] = returned[:, h * base : (h + 1) * base]

        def cell_ids(s):
            return jnp.concatenate(
                [recv_ref[0, 0, k, s : s + 1, :] for k in range(capacity)], axis=1)

        for s in range(air_groups):
            idx = cell_ids(s)
            at = slice(s * span, (s + 1) * span)
            low = as_rows(idx & (base - 1), 16)
            for t in range(base // 16):
                lowmat[t * 16 : (t + 1) * 16, at] = low_hot(low, t)
            found = mm(ret_bf[...], lowmat[:, at])
            high_of = jnp.broadcast_to(idx >> bits, (ret_pad, span))
            looked = jnp.zeros((ret_pad, span), F32)
            for h in range(highs):
                looked = jnp.where(high_of == h, found[h * ret_pad : (h + 1) * ret_pad], looked)
            for k in range(capacity):
                down_out[s, k] = looked[:, k * block : (k + 1) * block].astype(BF)
            down[s].start()
        spread[...] = jnp.zeros(spread.shape, BF)
        base_p = base_of(omat0.shape[0])
        tiles = cells // width

        def build(c, mat, marks):
            at = pl.ds(pl.multiple_of(c * width, width), width)
            rows_in = [onbr_ref[0, k, :, at] for k in range(neighbours)]
            counts_matrix(mat, marks, rows_in, base_p, slice(0, width))

        def product(c, mat):
            at = pl.ds(pl.multiple_of(c * width, width), width)
            mean = mm(opool[...], mat[...]) * (1.0 / neighbours)
            state = sea_ref[0, 0, :, at]
            sea_out[0, 0, :, at] = state + omix_ref[0, :, at] * (mean - state)

        build(0, omat0, high)
        take_halo(opool, levels_o, cells)

        def pair(i, _):
            product(2 * i, omat0)
            build(2 * i + 1, omat1, high1)
            product(2 * i + 1, omat1)
            build(2 * i + 2, omat0, high)
            return _

        lax.fori_loop(0, tiles // 2 - 1, pair, 0)
        product(tiles - 2, omat0)
        build(tiles - 1, omat1, high1)
        product(tiles - 1, omat1)
        flux = jnp.zeros((highs * field_pad, base), F32)
        for s in range(air_groups):
            pltpu.make_async_remote_copy(
                src_ref=up_out.at[s], dst_ref=up_in.at[s], send_sem=x_send.at[s],
                recv_sem=x_recv.at[s], device_id={"grp": first + s}).wait_recv()
            at = slice(s * span, (s + 1) * span)
            arrived = up_in[s].astype(F32)
            high_of = jnp.broadcast_to(cell_ids(s) >> bits, (fields, span))
            for h in range(highs):
                spread[h * field_pad : h * field_pad + fields, at] = (
                    jnp.where(high_of == h, arrived, 0.0).astype(BF))
            flux = flux + lax.dot_general(
                spread[:, at], lowmat[:, at], NT, preferred_element_type=F32)
        for h in range(highs):
            at = slice(h * base, (h + 1) * base)
            sea_out[0, 0, :, at] += lax.dot_general(
                force_ref[...], flux[h * field_pad : h * field_pad + fields],
                (((0,), (0,)), ((), ())), precision=EXACT, preferred_element_type=F32)
        for p in range(partners):
            down[p].wait_send()


def solution(mesh):
    groups, devs = mesh.shape["grp"], mesh.shape["dev"]
    in_specs = (
        P("grp", "dev", None, None), P("grp", "dev", None, None), P("grp", "dev", None),
        P("grp", "dev", None), P(), P("grp", "dev", None), P("grp", "dev", None),
        P("grp", "dev", None, None), P("grp", "dev", None, None, None),
        P("grp", "dev", None, None), P("grp", "dev", None, None), P("grp", "dev", None),
        P("grp", "dev", None), P(), P(),
    )
    out_specs = (P("grp", "dev", None, None),) * 3

    def on_device(*args):
        args = list(args)
        args[7] = args[7].transpose(0, 1, 3, 2)
        args[8] = args[8].transpose(0, 1, 3, 2, 4)
        args[10] = args[10].transpose(0, 2, 1, 3)
        args[13] = args[13].T
        air, anbr, asend, _, fw, _, mw, owner, recv, sea, onbr, _, _, _, ret = args
        levels_a, columns = air.shape[2:]
        levels_o, cells = sea.shape[2:]
        half = asend.shape[2] // 2
        capacity, air_groups, block = recv.shape[2:]
        sea_groups = groups - air_groups
        fields, ret_fields = fw.shape[0], ret.shape[0]
        ret_pad = -(-ret_fields // 16) * 16
        row_count = mw.shape[2]
        pool_a, pool_o = columns + 2 * half, cells + 2 * half
        width = 256
        base, span = base_of(cells), air_groups * capacity * block
        deep = max(
            anbr.shape[2] * (pool_a // base_of(pool_a)),
            onbr.shape[1] * (pool_o // base_of(pool_o)),
        )
        vmem = pl.BlockSpec(memory_space=pltpu.VMEM)
        smem = pl.BlockSpec(memory_space=pltpu.SMEM)
        ins = [vmem] * 15
        ins[7] = smem
        levels = max(levels_a, levels_o)
        V = pltpu.VMEM
        scratch = [
            V((2, levels, half), BF), V((2, levels, half), BF),
            V((levels_a, pool_a), BF), V((levels_o, pool_o), BF),
            V((pool_a, columns), BF), V((pool_o, width), BF), V((pool_o, width), BF),
            V((columns, row_count), BF), V((base, span), BF),
            V((cells // base * (-(-fields // 16) * 16), span), BF),
            V((deep, 16, width), BF), V((deep, 16, width), BF),
            V((owner.shape[3], fields, block), F32),
            V((sea_groups, fields, capacity * block), BF),
            V((air_groups, fields, capacity * block), BF),
            V((air_groups, capacity, ret_pad, block), BF),
            V((sea_groups, capacity, ret_pad, block), BF),
            V((ret_pad, levels_o), F32),
            V((max(4 * ret_pad, 2 * fields), max(row_count, columns)), BF),
            V((cells // base * ret_pad, base), BF),
            pltpu.SemaphoreType.DMA((2,)), pltpu.SemaphoreType.DMA((2,)),
            pltpu.SemaphoreType.DMA((air_groups,)), pltpu.SemaphoreType.DMA((air_groups,)),
        ]
        air_next, sea_next, back = pl.pallas_call(
            functools.partial(kernel, (groups, devs, air_groups)),
            out_shape=(
                jax.ShapeDtypeStruct(air.shape, F32),
                jax.ShapeDtypeStruct(sea.shape, F32),
                jax.ShapeDtypeStruct((1, ret_fields, 1, columns), F32),
            ),
            in_specs=ins,
            out_specs=(vmem,) * 3,
            scratch_shapes=scratch,
            compiler_params=pltpu.CompilerParams(
                collective_id=0, has_side_effects=True, vmem_limit_bytes=60 * 1024 * 1024),
            name="couple",
        )(*args)
        return air_next, sea_next, back.transpose(0, 2, 1, 3)

    return jax.shard_map(
        on_device, mesh=mesh, in_specs=in_specs, out_specs=out_specs, check_vma=False)
```
